32 devices in a mesh: depth: 8 (over z, core), image: 4 (over y, x).
Axes of the slice: x: 2, y: 2, z: 4, core: 2. Of those that a mesh axis runs over, the one named last changes fastest.
Arguments:
- level_set: float32 [128, 256, 512], P('depth', 'image'), may hold values from -6 to 6
- velocity: float32 [3, 128, 256, 512], P(None, 'depth', 'image'), may hold values from -1 to 1
- view_flag: int32 [8], replicated, may hold values from 0 to 1
- slab_rank: int32 [8], replicated, may hold values from 0 to 7, each once
Outputs:
- image_first: float32 [4, 256, 512], P(None, 'image', 'depth')
- image_second: float32 [4, 256, 512], P(None, 'image', 'depth')
- level_next: float32 [128, 256, 512], P('depth', 'image')
The draws below stay inside these ranges and needn't reach their ends.
Inputs may be any that keep to these rules, and one draw needn't show every extreme that they name: `slab_rank`: each of 0 to 7 once.
All inputs are finite; a program needn't handle non-finite values.
Results may differ from the reference program's by a relative error of at most 0.00013.
Values sent between devices are 32-bit elements; how exact they have to be, the bound alone decides.
No kernel may reach another device: no remote copies, remote signals or barrier semaphores. Data moves between devices by JAX's collectives and lax.ppermute only.
A program may use at most 64 MiB of HBM per device.

```python
import jax
import jax.numpy as jnp
from jax import lax

CZ = 16
STEPS = 4
NZ = 128
NX = 256
NY = 512
N_DEPTH = 8


def plant(entries, stream_key, least, high):
    spot = [jax.random.randint(jax.random.fold_in(stream_key, axis), (), 0, length) for axis, length in enumerate(entries.shape)]
    main_axis = entries.shape.index(max(entries.shape))
    neighbour = spot[:main_axis] + [(spot[main_axis] + 1) % entries.shape[main_axis]] + spot[main_axis + 1:]
    return entries.at[tuple(spot)].set(least).at[tuple(neighbour)].set(high)


def levels(rng, extent, pieces, low, top_value):
    level, own = 1.0, jax.random.fold_in(rng, 6)
    for dim, shards_of in pieces:
        draws = jnp.exp(jax.random.uniform(jax.random.fold_in(own, dim), (shards_of,), jnp.float32, low / len(pieces), top_value / len(pieces)))
        level = level * jnp.repeat(draws, extent[dim] // shards_of).reshape([-1 if axis == dim else 1 for axis in range(len(extent))])
    return level


def scatter_about(key, extent, scale, most, cuts=(), held_as=jnp.bfloat16):
    factor_of = levels(key, extent, cuts, -0.22, 0.18) if cuts else 1.0
    array = jax.random.normal(key, extent, jnp.float32) * scale * factor_of
    return jnp.minimum(jnp.maximum(array, -most), most).astype(held_as)


def setup_inputs(seed: int = 0) -> dict:
    seeds = jax.random.split(jax.random.key(seed), 5)
    return {
        "level_set": scatter_about(seeds[0], (NZ, NX, NY), 1.0, 6.0, ((0, 8), (1, 4)), jnp.float32),
        "velocity": jnp.clip(jax.random.uniform(seeds[1], (3, NZ, NX, NY), jnp.float32, -1.0, 1.0) * levels(seeds[1], (3, NZ, NX, NY), ((1, 8), (2, 4)), -0.4, 0.0), -1.0, 1.0),
        "view_flag": plant(jax.random.randint(seeds[2], (N_DEPTH,), 0, 2), jax.random.fold_in(seeds[2], 1), 0, 1).astype(jnp.int32),
        "slab_rank": jax.random.permutation(seeds[3], N_DEPTH).astype(jnp.int32),
    }


step_size = 0.3


def upwind(padded):
    center = padded[1:-1, 1:-1, 1:-1]
    lows = (padded[:-2, 1:-1, 1:-1], padded[1:-1, :-2, 1:-1], padded[1:-1, 1:-1, :-2])
    highs = (padded[2:, 1:-1, 1:-1], padded[1:-1, 2:, 1:-1], padded[1:-1, 1:-1, 2:])
    return center, lows, highs


def advect(center, lows, highs, velocity):
    rate = jnp.zeros_like(center)
    for k in range(3):
        speed = velocity[k]
        rate = rate + jnp.maximum(speed, 0.0) * (center - lows[k]) + jnp.minimum(speed, 0.0) * (highs[k] - center)
    return center - step_size * rate


def render_slabs(field, flags, scale):
    density = scale * jnp.exp(-field * field)
    colour = jnp.stack([jax.nn.sigmoid(2.0 * field), jnp.exp(-field * field), jax.nn.sigmoid(-2.0 * field)], axis=-4)
    running = jnp.cumsum(density, axis=-3)
    totals = running[..., -1:, :, :]
    before = jnp.where(flags[:, None, None, None] == 0, running - density, totals - running)
    weight = jnp.exp(-before) * (1.0 - jnp.exp(-density))
    partial_colour = jnp.sum(weight[..., None, :, :, :] * colour, axis=-3)
    return partial_colour, -totals[..., 0, :, :]


def composite(partial_colour, log_trans, slab_rank):
    earlier_mask = (slab_rank[None, :] < slab_rank[:, None]).astype(jnp.float32)
    earlier = jnp.einsum('de,exy->dxy', earlier_mask, log_trans, precision=lax.Precision.HIGHEST)
    rgb = jnp.sum(jnp.exp(earlier)[:, None] * partial_colour, axis=0)
    alpha = 1.0 - jnp.exp(jnp.sum(log_trans, axis=0))
    return jnp.concatenate([rgb, alpha[None]], axis=0)


def frame_image(field, view_flag, slab_rank):
    slabs = field.reshape(N_DEPTH, CZ, NX, NY)
    partial_colour, log_trans = render_slabs(slabs, view_flag, 2.0 / NZ)
    return composite(partial_colour, log_trans, slab_rank)


def reference(level_set, velocity, view_flag, slab_rank):
    image_first = frame_image(level_set, view_flag, slab_rank)
    field = level_set
    for step in range(STEPS):
        center, lows, highs = upwind(jnp.pad(field, 1))
        field = advect(center, lows, highs, velocity)
    image_second = frame_image(field, view_flag, slab_rank)
    return image_first, image_second, field
```

```python
import functools

import jax
import jax.numpy as jnp
from jax import lax
from jax.experimental import pallas as pl
from jax.experimental.pallas import tpu as pltpu
from jax.sharding import PartitionSpec as P

STEPS = 4
step_size = 0.3
LANES = 128
SUB = 8
W = STEPS

VMEM = pl.BlockSpec(memory_space=pltpu.VMEM)
SMEM = pl.BlockSpec(memory_space=pltpu.SMEM)
FAR = pl.BlockSpec(memory_space=pltpu.HBM)


def f32(*shape):
    return jax.ShapeDtypeStruct(shape, jnp.float32)


def near(*shape):
    return pltpu.VMEM(shape, jnp.float32)


def resident(*arrays):
    return [pltpu.with_memory_space_constraint(a, pltpu.VMEM) for a in arrays]


def params(mib=None):
    if mib is None:
        return pltpu.CompilerParams()
    return pltpu.CompilerParams(vmem_limit_bytes=mib * 2**20)


def distant(*arrays):
    return [pltpu.with_memory_space_constraint(a, pltpu.HBM) for a in arrays]


def low_half(shape):
    return lax.broadcasted_iota(jnp.int32, shape, len(shape) - 2) < W


def is_even():
    return lax.rem(lax.axis_index("depth"), 2) == 0


def depth_pack_kernel(level, vel, cross, inner, sems):
    planes = level.shape[0]
    even = is_even()
    copies = []
    for n, (out, to_low) in enumerate(((cross, even), (inner, jnp.logical_not(even)))):
        z0 = jnp.where(to_low, 0, planes - W)
        v0 = jnp.where(to_low, 0, planes - W + 1)
        copies.append(pltpu.make_async_copy(level.at[pl.ds(z0, W)], out.at[pl.ds(0, W)], sems.at[n, 0]))
        for k in range(3):
            copies.append(
                pltpu.make_async_copy(
                    vel.at[k, pl.ds(v0, W - 1)],
                    out.at[pl.ds(W + (W - 1) * k, W - 1)],
                    sems.at[n, k + 1],
                )
            )
    for c in copies:
        c.start()
    for c in copies:
        c.wait()


def depth_pack(level, vel):
    planes, rows, cols = level.shape
    shape = near(W + 3 * (W - 1), rows, cols)
    return pl.pallas_call(
        depth_pack_kernel,
        out_shape=(shape, shape),
        in_specs=[FAR, FAR],
        out_specs=(VMEM, VMEM),
        scratch_shapes=[pltpu.SemaphoreType.DMA((2, 4))],
        compiler_params=params(6),
        name="depth_pack",
    )(*distant(level, vel))


def image_pack_kernel(level, vel, up1, down1, up2, down2, lev, ve, sems):
    planes, rows, _ = level.shape
    copies = []
    for s, r0 in enumerate((0, rows - SUB)):
        copies.append(pltpu.make_async_copy(level.at[:, pl.ds(r0, SUB), :], lev.at[s], sems.at[s, 0]))
        copies.append(pltpu.make_async_copy(vel.at[:, :, pl.ds(r0, SUB), :], ve.at[s], sems.at[s, 1]))
    for c in copies:
        c.start()
    for c in copies:
        c.wait()

    def emit(z, slot, up, down):
        low = low_half(lev.shape[-2:])
        half = lambda a: pltpu.roll(a, W, 0)
        down[slot, 0:SUB] = jnp.where(low, lev[0, z], half(ve[0, 0, z]))
        down[slot, SUB : 2 * SUB] = jnp.where(low, ve[0, 1, z], half(ve[0, 2, z]))
        up[slot, 0:SUB] = jnp.where(low, half(ve[1, 0, z]), lev[1, z])
        up[slot, SUB : 2 * SUB] = jnp.where(low, half(ve[1, 2, z]), ve[1, 1, z])

    def outer(j, c):
        emit(jnp.where(j < W, j, j + planes - 2 * W), j, up1, down1)
        return c

    def inner(j, c):
        emit(j + W, j, up2, down2)
        return c

    lax.fori_loop(0, 2 * W, outer, 0)
    lax.fori_loop(0, planes - 2 * W, inner, 0)


def image_pack(level, vel):
    planes, rows, cols = level.shape
    a = near(2 * W, 2 * SUB, cols)
    b = near(planes - 2 * W, 2 * SUB, cols)
    return pl.pallas_call(
        image_pack_kernel,
        out_shape=(a, a, b, b),
        in_specs=[FAR, FAR],
        out_specs=(VMEM,) * 4,
        scratch_shapes=[
            pltpu.VMEM((2, planes, SUB, cols), jnp.float32),
            pltpu.VMEM((2, 3, planes, SUB, cols), jnp.float32),
            pltpu.SemaphoreType.DMA((2, 2)),
        ],
        compiler_params=params(6),
        name="image_pack",
    )(*distant(level, vel))


def row_halos(hi, lo, slot):
    low = low_half((SUB, hi.shape[-1]))
    h0, h1, l0, l1 = hi[slot, 0:SUB], hi[slot, SUB : 2 * SUB], lo[slot, 0:SUB], lo[slot, SUB : 2 * SUB]
    return (
        jnp.where(low, h0, l0),
        pltpu.roll(jnp.where(low, l0, h0), W, 0),
        jnp.where(low, h1, l1),
        pltpu.roll(jnp.where(low, l1, h1), W, 0),
    )


def corner_pack_kernel(hi, lo, cross, inner):
    even = is_even()
    for out, to_low in ((cross, even), (inner, jnp.logical_not(even))):
        s0 = jnp.where(to_low, 0, W)
        first = jnp.where(to_low, 0, 1)
        for j in range(W):
            tiles = row_halos(hi, lo, s0 + j)
            out[j] = tiles[0]
            at = j - first

            @pl.when((at >= 0) & (at < W - 1))
            def _():
                for k in range(3):
                    out[W + (W - 1) * k + at] = tiles[k + 1]


def corner_pack(hi, lo):
    shape = near(W + 3 * (W - 1), SUB, hi.shape[-1])
    return pl.pallas_call(
        corner_pack_kernel,
        out_shape=(shape, shape),
        in_specs=[VMEM, VMEM],
        out_specs=(VMEM, VMEM),
        compiler_params=params(6),
        name="corner_pack",
    )(*resident(hi, lo))


def render(field, planes, rows, cols, flag, scale, out, sums):
    reverse = flag != 0
    sign = jnp.where(reverse, 1.0, -1.0).astype(jnp.float32)

    def tile(i, c):
        r0 = pl.multiple_of(i * SUB, SUB)
        total = jnp.zeros((SUB, cols), jnp.float32)
        last = jnp.ones((SUB, cols), jnp.float32)
        q = jnp.zeros((SUB, cols), jnp.float32)
        g = jnp.zeros((SUB, cols), jnp.float32)
        step = sign * scale
        for z in range(planes):
            f = field[z, pl.ds(r0, SUB), :]
            e = jnp.exp(-f * f)
            total = total + e * step
            now = jnp.exp(total)
            weight = now - last
            last = now
            q = q + weight * jnp.tanh(f)
            g = g + weight * e
        logs = -sign * total
        factor = jnp.where(reverse, jnp.exp(logs), -1.0)
        sums[0, pl.ds(r0, SUB), :] = q * factor
        sums[1, pl.ds(r0, SUB), :] = g * factor
        sums[2, pl.ds(r0, SUB), :] = logs
        return c

    lax.fori_loop(0, rows // SUB, tile, 0)


def spread(sums, out):
    _, rows, cols = sums.shape
    dests = out.shape[0]
    width = cols // dests
    groups = LANES // width
    part = rows // groups
    lane = lax.broadcasted_iota(jnp.int32, (part, LANES), 1)
    for d in range(dests):
        j, offset = divmod(d * width, LANES)
        for ch in range(3):
            value = None
            for n in range(groups):
                piece = sums[ch, n * part : (n + 1) * part, j * LANES : (j + 1) * LANES]
                shift = (n * width - offset) % LANES
                if shift:
                    piece = pltpu.roll(piece, shift, 1)
                value = piece if value is None else jnp.where(lane < n * width, value, piece)
            out[d, ch * part : (ch + 1) * part, :] = value


def first_kernel(flag, level, out, ext_f, sums, sem, *, scale):
    planes, rows, cols = level.shape
    a = pltpu.make_async_copy(level, ext_f.at[pl.ds(0, planes), pl.ds(0, rows), :], sem)
    a.start()
    a.wait()
    render(ext_f, planes, rows, cols, flag[lax.axis_index("depth")], scale, out, sums)
    spread(sums, out)


def first(level, flag, scale, dests):
    planes, rows, cols = level.shape
    ext = (planes + 2 * W, rows + SUB, cols)
    return pl.pallas_call(
        functools.partial(first_kernel, scale=scale),
        out_shape=(f32(dests, 3 * rows * cols // dests // LANES, LANES), near(*ext)),
        in_specs=[SMEM, FAR],
        out_specs=(VMEM, VMEM),
        scratch_shapes=[pltpu.VMEM((3, rows, cols), jnp.float32), pltpu.SemaphoreType.DMA],
        compiler_params=params(6),
        name="first",
    )(flag, *distant(level))


def side(tiles, j, lane, up):
    n = len(tiles)
    own = pltpu.roll(tiles[j], 1 if not up else LANES - 1, 1)
    k = j + 1 if up else j - 1
    if 0 <= k < n:
        other = pltpu.roll(tiles[k], 1 if not up else LANES - 1, 1)
    else:
        other = jnp.zeros_like(own)
    return jnp.where(lane == (LANES - 1 if up else 0), other, own)


def second_kernel(
    flag, ext_f, vel, cross, inner, ccross, cinner, hi1, lo1, hi2, lo2,
    out, level_out, f0, other, edge, sums, sem, *, scale,
):
    layers, all_rows, cols = ext_f.shape
    planes, rows = layers - 2 * W, all_rows - SUB
    even = is_even()

    for src, corner, low in ((cross, ccross, even), (inner, cinner, jnp.logical_not(even))):
        zf = jnp.where(low, planes + W, planes)
        for j in range(W):
            f0[zf + j, 0:rows] = src[j]
            f0[zf + j, rows : rows + SUB] = corner[j]

    def fill(z, slot, hi, lo):
        tiles = row_halos(hi, lo, slot)
        f0[z, rows : rows + SUB] = tiles[0]
        for k in range(3):
            edge[k, z] = tiles[k + 1]

    def fill_outer(j, c):
        fill(jnp.where(j < W, j, j + planes - 2 * W), j, hi1, lo1)
        return c

    def fill_inner(j, c):
        fill(j + W, j, hi2, lo2)
        return c

    lax.fori_loop(0, 2 * W, fill_outer, 0)
    lax.fori_loop(0, planes - 2 * W, fill_inner, 0)

    nt = all_rows // SUB
    nl = cols // LANES

    def layer(src, dst, z, row_tiles, speed):
        zi = jnp.where(z < 0, z + layers, z)
        zl = jnp.where(z < 1, z - 1 + layers, z - 1)
        zh = jnp.where(z < -1, z + 1 + layers, z + 1)
        sub = lax.broadcasted_iota(jnp.int32, (SUB, LANES), 0)
        lane = lax.broadcasted_iota(jnp.int32, (SUB, LANES), 1)
        first_sub = sub == 0
        last_sub = sub == SUB - 1
        for i in range(row_tiles):
            r = slice(i * SUB, (i + 1) * SUB)
            ru = slice((i + 1) % nt * SUB, ((i + 1) % nt + 1) * SUB)
            rd = slice((i - 1) % nt * SUB, ((i - 1) % nt + 1) * SUB)
            tiles = [src[zi, r, j * LANES : (j + 1) * LANES] for j in range(nl)]
            for j in range(nl):
                js = slice(j * LANES, (j + 1) * LANES)
                f = tiles[j]
                below = src[zi, rd, js]
                above = src[zi, ru, js]
                lows = (
                    lambda: src[zl, r, js],
                    lambda: jnp.where(first_sub, pltpu.roll(below, 1, 0), pltpu.roll(f, 1, 0)),
                    lambda: side(tiles, j, lane, False),
                )
                highs = (
                    lambda: src[zh, r, js],
                    lambda: jnp.where(last_sub, pltpu.roll(above, SUB - 1, 0), pltpu.roll(f, SUB - 1, 0)),
                    lambda: side(tiles, j, lane, True),
                )
                rate = None
                for k in range(3):
                    u = speed(k, i, js)
                    upwind = jnp.where(u > 0.0, lows[k](), highs[k]())
                    term = jnp.abs(u) * (upwind - f)
                    rate = term if rate is None else rate + term
                dst[zi, r, js] = f + step_size * rate

    def step(src, dst, t):
        reach = STEPS - t
        row_tiles = nt if reach else rows // SUB
        own_tiles = rows // SUB

        def own(z, c):
            def speed(k, i, js):
                if i == own_tiles:
                    return edge[k, z, :, js]
                return vel[k, z, i * SUB : (i + 1) * SUB, js]

            layer(src, dst, z, row_tiles, speed)
            return c

        lax.fori_loop(0, planes, own, 0)

        for halo, corner, low in ((cross, ccross, even), (inner, cinner, jnp.logical_not(even))):
            skip = jnp.where(low, W - 1 - reach, 0)
            base = jnp.where(low, -reach, planes)

            def outside(n, c):
                def speed(k, i, js):
                    at = W + (W - 1) * k + skip + n
                    if i == own_tiles:
                        return corner[at, :, js]
                    return halo[at, i * SUB : (i + 1) * SUB, js]

                layer(src, dst, base + n, row_tiles, speed)
                return c

            if reach:
                lax.fori_loop(0, reach, outside, 0)

    src, dst = f0, other
    for t in range(1, STEPS + 1):
        step(src, dst, t)
        src, dst = dst, src

    store = pltpu.make_async_copy(src.at[pl.ds(0, planes), pl.ds(0, rows), :], level_out, sem)
    store.start()
    render(src, planes, rows, cols, flag[lax.axis_index("depth")], scale, out, sums)
    spread(sums, out)
    store.wait()


def second(flag, ext_f, vel, halos, scale, dests):
    layers, all_rows, cols = ext_f.shape
    planes, rows = layers - 2 * W, all_rows - SUB
    return pl.pallas_call(
        functools.partial(second_kernel, scale=scale),
        out_shape=(
            f32(dests, 3 * rows * cols // dests // LANES, LANES),
            pltpu.HBM((planes, rows, cols), jnp.float32),
            near(*ext_f.shape),
        ),
        in_specs=[SMEM] + [VMEM] * 10,
        out_specs=(VMEM, FAR, VMEM),
        input_output_aliases={1: 2},
        scratch_shapes=[
            pltpu.VMEM(ext_f.shape, jnp.float32),
            pltpu.VMEM((3, planes, SUB, cols), jnp.float32),
            pltpu.VMEM((3, rows, cols), jnp.float32),
            pltpu.SemaphoreType.DMA,
        ],
        compiler_params=params(10),
        name="second",
    )(flag, *resident(ext_f, vel, *halos))[:2]


def composite_kernel(rank, parts, out):
    dests, stacked, _ = parts.shape
    part = stacked // 3
    _, rows, width = out.shape
    groups = rows // part
    for i in range(part // SUB):
        r = slice(i * SUB, (i + 1) * SUB)
        logs = [parts[e, 2 * part + i * SUB : 2 * part + (i + 1) * SUB, :] for e in range(dests)]
        q = g = total = None
        for b in range(dests):
            earlier = jnp.zeros((SUB, LANES), jnp.float32)
            for e in range(dests):
                if e != b:
                    earlier = earlier + jnp.where(rank[e] < rank[b], 1.0, 0.0) * logs[e]
            front = jnp.exp(earlier)
            qb = front * parts[b, r, :]
            gb = front * parts[b, part + i * SUB : part + (i + 1) * SUB, :]
            q = qb if q is None else q + qb
            g = gb if g is None else g + gb
            total = logs[b] if total is None else total + logs[b]
        alpha = 1.0 - jnp.exp(total)
        for ch, value in enumerate((0.5 * (alpha + q), g, 0.5 * (alpha - q), alpha)):
            for n in range(groups):
                piece = pltpu.roll(value, (LANES - n * width) % LANES, 1) if n else value
                out[ch, n * part + i * SUB : n * part + (i + 1) * SUB, :] = piece[:, :width]


def composite(rank, parts, rows, width):
    return pl.pallas_call(
        composite_kernel,
        out_shape=f32(4, rows, width),
        in_specs=[SMEM, VMEM],
        out_specs=VMEM,
        compiler_params=params(6),
        name="composite",
    )(rank, *resident(parts))


def local(level_set, velocity, view_flag, slab_rank):
    planes, rows, cols = level_set.shape
    depth = lax.axis_size("depth")
    image = lax.axis_size("image")
    scale = 2.0 / (planes * depth)
    width = cols // depth

    swap_inner = [(i, i ^ 1) for i in range(depth)]
    swap_cross = [p for i in range(1, depth - 1, 2) for p in ((i, i + 1), (i + 1, i))]
    up = [(i, i + 1) for i in range(image - 1)]
    down = [(b, a) for a, b in up]

    cross, inner = depth_pack(level_set, velocity)
    cross = lax.ppermute(cross, "depth", swap_cross)
    inner = lax.ppermute(inner, "depth", swap_inner)
    up1, down1, up2, down2 = image_pack(level_set, velocity)
    lo1 = lax.ppermute(up1, "image", up)
    hi1 = lax.ppermute(down1, "image", down)
    lo2 = lax.ppermute(up2, "image", up)
    hi2 = lax.ppermute(down2, "image", down)
    ccross, cinner = corner_pack(hi1, lo1)
    ccross = lax.ppermute(ccross, "depth", swap_cross)
    cinner = lax.ppermute(cinner, "depth", swap_inner)

    packed, ext_f = first(level_set, view_flag, scale, depth)
    parts = lax.all_to_all(packed, "depth", 0, 0, tiled=True)
    halos = (cross, inner, ccross, cinner, hi1, lo1, hi2, lo2)
    packed2, level_next = second(view_flag, ext_f, velocity, halos, scale, depth)
    parts2 = lax.all_to_all(packed2, "depth", 0, 0, tiled=True)
    image_first = composite(slab_rank, parts, rows, width)
    image_second = composite(slab_rank, parts2, rows, width)
    return (image_first, image_second, level_next)


def solution(mesh):
    placed = (P("depth", "image", None), P(None, "depth", "image", None), P(), P())
    return jax.shard_map(
        local,
        mesh=mesh,
        in_specs=placed,
        out_specs=(P(None, "image", "depth"), P(None, "image", "depth"), P("depth", "image", None)),
        check_vma=False,
    )
```

```python
import functools

import jax
import jax.numpy as jnp
from jax import lax
from jax.experimental import pallas as pl
from jax.experimental.pallas import tpu as pltpu
from jax.sharding import PartitionSpec as P


STEPS = 4
step_size = 0.3
LANES = 128
SUB = 8
W = STEPS

VMEM = pl.BlockSpec(memory_space=pltpu.VMEM)
SMEM = pl.BlockSpec(memory_space=pltpu.SMEM)
FAR = pl.BlockSpec(memory_space=pltpu.HBM)
LOOSE = pl.BlockSpec(memory_space=pl.ANY)


def f32(*shape):
    return jax.ShapeDtypeStruct(shape, jnp.float32)


def near(*shape):
    return pltpu.VMEM(shape, jnp.float32)


def resident(*arrays):
    return [pltpu.with_memory_space_constraint(a, pltpu.VMEM) for a in arrays]


def params(mib=None):
    if mib is None:
        return pltpu.CompilerParams()
    return pltpu.CompilerParams(vmem_limit_bytes=mib * 2**20)


def distant(*arrays):
    return [pltpu.with_memory_space_constraint(a, pltpu.HBM) for a in arrays]


def is_even():
    return lax.rem(lax.axis_index("depth"), 2) == 0


def depth_pack_kernel(level, vel, cross, inner, sems):
    planes = level.shape[0]
    even = is_even()
    copies = []
    for n, (out, to_low) in enumerate(((cross, even), (inner, jnp.logical_not(even)))):
        z0 = jnp.where(to_low, 0, planes - W)
        v0 = jnp.where(to_low, 0, planes - W + 1)
        copies.append(pltpu.make_async_copy(level.at[pl.ds(z0, W)], out.at[pl.ds(0, W)], sems.at[n, 0]))
        for k in range(3):
            copies.append(
                pltpu.make_async_copy(
                    vel.at[k, pl.ds(v0, W - 1)],
                    out.at[pl.ds(W + (W - 1) * k, W - 1)],
                    sems.at[n, k + 1],
                )
            )
    for c in copies:
        c.start()
    for c in copies:
        c.wait()


def depth_pack(level, vel):
    _, rows, cols = level.shape
    shape = near(W + 3 * (W - 1), rows, cols)
    return pl.pallas_call(
        depth_pack_kernel,
        out_shape=(shape, shape),
        in_specs=[FAR, FAR],
        out_specs=(VMEM, VMEM),
        scratch_shapes=[pltpu.SemaphoreType.DMA((2, 4))],
        compiler_params=params(6),
        name="depth_pack",
    )(*distant(level, vel))


HALO_ROWS = W + 3 * (W - 1)


def row_span(z, k=None):
    start = z * HALO_ROWS + (0 if k is None else W + (W - 1) * k)
    return slice(start, start + (W if k is None else W - 1))


def image_pack_kernel(level, vel, up, down, lev, ve, sems):
    planes, rows, _ = level.shape
    copies = []
    for s, r0 in enumerate((0, rows - SUB)):
        copies.append(pltpu.make_async_copy(level.at[:, pl.ds(r0, SUB), :], lev.at[s], sems.at[s, 0]))
        copies.append(pltpu.make_async_copy(vel.at[:, :, pl.ds(r0, SUB), :], ve.at[s], sems.at[s, 1]))
    for c in copies:
        c.start()
    for c in copies:
        c.wait()

    for z in range(planes):
        down[row_span(z)] = lev[0, z, 0:W]
        up[row_span(z)] = lev[1, z, SUB - W : SUB]
        for k in range(3):
            down[row_span(z, k)] = ve[0, k, z, 0 : W - 1]
            up[row_span(z, k)] = ve[1, k, z, SUB - W + 1 : SUB]


def image_pack(level, vel):
    planes, _, cols = level.shape
    shape = near(planes * HALO_ROWS, cols)
    return pl.pallas_call(
        image_pack_kernel,
        out_shape=(shape, shape),
        in_specs=[FAR, FAR],
        out_specs=(VMEM, VMEM),
        scratch_shapes=[
            pltpu.VMEM((2, planes, SUB, cols), jnp.float32),
            pltpu.VMEM((2, 3, planes, SUB, cols), jnp.float32),
            pltpu.SemaphoreType.DMA((2, 2)),
        ],
        compiler_params=params(6),
        name="image_pack",
    )(*distant(level, vel))


def put_row_halos(field, speeds, hi, lo, z):
    field[0:W] = hi[row_span(z)]
    field[W:SUB] = lo[row_span(z)]
    for k, speed in enumerate(speeds):
        speed[...] = jnp.zeros(speed.shape, jnp.float32)
        speed[0 : W - 1] = hi[row_span(z, k)]
        speed[SUB - W + 1 : SUB] = lo[row_span(z, k)]


def corner_pack_kernel(hi, lo, cross, inner):
    planes = hi.shape[0] // HALO_ROWS
    even = is_even()

    def pack(low, high):
        for out, first, skip in ((low, 0, 0), (high, planes - W, 1)):
            for j in range(W):
                at = j - skip
                speeds = []
                if 0 <= at < W - 1:
                    speeds = [out.at[W + (W - 1) * k + at] for k in range(3)]
                put_row_halos(out.at[j], speeds, hi, lo, first + j)

    @pl.when(even)
    def _():
        pack(cross, inner)

    @pl.when(jnp.logical_not(even))
    def _():
        pack(inner, cross)


def corner_pack(hi, lo):
    shape = near(W + 3 * (W - 1), SUB, hi.shape[-1])
    return pl.pallas_call(
        corner_pack_kernel,
        out_shape=(shape, shape),
        in_specs=[VMEM, VMEM],
        out_specs=(VMEM, VMEM),
        compiler_params=params(6),
        name="corner_pack",
    )(*resident(hi, lo))


def render(field, planes, rows, cols, flag, scale, sums):
    reverse = flag != 0
    sign = jnp.where(reverse, 1.0, -1.0).astype(jnp.float32)

    def tile(i, c):
        r0 = pl.multiple_of(i * SUB, SUB)
        total = jnp.zeros((SUB, cols), jnp.float32)
        last = jnp.ones((SUB, cols), jnp.float32)
        q = jnp.zeros((SUB, cols), jnp.float32)
        g = jnp.zeros((SUB, cols), jnp.float32)
        step = sign * scale
        for z in range(planes):
            f = field[z, pl.ds(r0, SUB), :]
            e = jnp.exp(-f * f)
            total = total + e * step
            now = jnp.exp(total)
            weight = now - last
            last = now
            q = q + weight * jnp.tanh(f)
            g = g + weight * e
        logs = -sign * total
        factor = jnp.where(reverse, jnp.exp(logs), -1.0)
        sums[0, pl.ds(r0, SUB), :] = q * factor
        sums[1, pl.ds(r0, SUB), :] = g * factor
        sums[2, pl.ds(r0, SUB), :] = logs
        return c

    lax.fori_loop(0, rows // SUB, tile, 0)


def spread(sums, out, stage, sem):
    _, rows, cols = sums.shape
    dests = out.shape[0]
    copies = []
    width = cols // dests
    groups = LANES // width
    part = rows // groups
    lane = lax.broadcasted_iota(jnp.int32, (part, LANES), 1)
    for d in range(dests):
        j, offset = divmod(d * width, LANES)
        for ch in range(3):
            value = None
            for n in range(groups):
                piece = sums[ch, n * part : (n + 1) * part, j * LANES : (j + 1) * LANES]
                shift = (n * width - offset) % LANES
                if shift:
                    piece = pltpu.roll(piece, shift, 1)
                value = piece if value is None else jnp.where(lane < n * width, value, piece)
            stage[d, ch * part : (ch + 1) * part, :] = value
        copies.append(pltpu.make_async_copy(stage.at[d], out.at[d], sem.at[d]))
        copies[-1].start()
    return copies


def first_kernel(flag, level, after, out, sums, stage, sent, *, scale):
    planes, rows, cols = level.shape
    render(level, planes, rows, cols, flag[lax.axis_index("depth")], scale, sums)
    for c in spread(sums, out, stage, sent):
        c.wait()


def first(level, flag, after, scale, dests):
    _, rows, cols = level.shape
    packed = (dests, 3 * rows * cols // dests // LANES, LANES)
    return pl.pallas_call(
        functools.partial(first_kernel, scale=scale),
        out_shape=pltpu.HBM(packed, jnp.float32),
        in_specs=[SMEM, VMEM, LOOSE],
        out_specs=FAR,
        scratch_shapes=[
            pltpu.VMEM((3, rows, cols), jnp.float32),
            pltpu.VMEM(packed, jnp.float32),
            pltpu.SemaphoreType.DMA((dests,)),
        ],
        compiler_params=params(6),
        name="first",
    )(flag, *resident(level), after)


def side(tiles, j, lane, up):
    n = len(tiles)
    own = pltpu.roll(tiles[j], 1 if not up else LANES - 1, 1)
    k = j + 1 if up else j - 1
    if 0 <= k < n:
        other = pltpu.roll(tiles[k], 1 if not up else LANES - 1, 1)
    else:
        other = jnp.zeros_like(own)
    return jnp.where(lane == (LANES - 1 if up else 0), other, own)


def layer(src, dst, z, row_tiles, speed):
    layers, all_rows, cols = src.shape
    nt = all_rows // SUB
    nl = cols // LANES
    zi = jnp.where(z < 0, z + layers, z)
    zl = jnp.where(z < 1, z - 1 + layers, z - 1)
    zh = jnp.where(z < -1, z + 1 + layers, z + 1)
    sub = lax.broadcasted_iota(jnp.int32, (SUB, LANES), 0)
    lane = lax.broadcasted_iota(jnp.int32, (SUB, LANES), 1)
    first_sub = sub == 0
    last_sub = sub == SUB - 1
    for i in range(row_tiles):
        r = slice(i * SUB, (i + 1) * SUB)
        ru = slice((i + 1) % nt * SUB, ((i + 1) % nt + 1) * SUB)
        rd = slice((i - 1) % nt * SUB, ((i - 1) % nt + 1) * SUB)
        tiles = [src[zi, r, j * LANES : (j + 1) * LANES] for j in range(nl)]
        for j in range(nl):
            js = slice(j * LANES, (j + 1) * LANES)
            f = tiles[j]
            below = src[zi, rd, js]
            above = src[zi, ru, js]
            lows = (
                lambda: src[zl, r, js],
                lambda: jnp.where(first_sub, pltpu.roll(below, 1, 0), pltpu.roll(f, 1, 0)),
                lambda: side(tiles, j, lane, False),
            )
            highs = (
                lambda: src[zh, r, js],
                lambda: jnp.where(last_sub, pltpu.roll(above, SUB - 1, 0), pltpu.roll(f, SUB - 1, 0)),
                lambda: side(tiles, j, lane, True),
            )
            rate = None
            for k in range(3):
                u = speed(k, i, js)
                upwind = jnp.where(u > 0.0, lows[k](), highs[k]())
                term = jnp.abs(u) * (upwind - f)
                rate = term if rate is None else rate + term
            dst[zi, r, js] = f + step_size * rate


def own_layer(src, dst, z, row_tiles, vel, edge):
    own_tiles = vel.shape[2] // SUB

    def speed(k, i, js):
        if i == own_tiles:
            return edge[k, z, :, js]
        return vel[k, z, i * SUB : (i + 1) * SUB, js]

    layer(src, dst, z, row_tiles, speed)


def early_kernel(
    level, speeds, cross, inner, hi, lo, after,
    f0, f1, vel, hcross, hinner, edge, sems, arrived,
):
    layers, all_rows, _ = f0.shape
    planes, rows = layers - 2 * W, all_rows - SUB
    even = is_even()

    streams = [
        pltpu.make_async_copy(speeds.at[:, z], vel.at[:, z], arrived.at[z]) for z in range(planes)
    ]
    copies = [streams[0], streams[-1]]
    for n, (src, halo, low) in enumerate(((cross, hcross, even), (inner, hinner, jnp.logical_not(even)))):
        zf = jnp.where(low, planes + W, planes)
        copies.append(
            pltpu.make_async_copy(
                src.at[pl.ds(0, W)], f0.at[pl.ds(zf, W), pl.ds(0, rows), :], sems.at[n, 0]
            )
        )
        copies.append(pltpu.make_async_copy(src.at[pl.ds(W, 3 * (W - 1))], halo, sems.at[n, 1]))
    for c in streams[1:-1] + copies:
        c.start()

    def fill(z, c):
        f0[z, 0:rows] = level[z]
        return c

    lax.fori_loop(0, planes, fill, 0)
    for z in range(planes):
        put_row_halos(f0.at[z, rows : rows + SUB], [edge.at[k, z] for k in range(3)], hi, lo, z)

    def arriving(z, c):
        pltpu.make_async_copy(speeds.at[:, z], vel.at[:, z], arrived.at[z]).wait()
        own_layer(f0, f1, z, all_rows // SUB, vel, edge)
        return c

    lax.fori_loop(1, planes - 1, arriving, 0)
    for c in copies:
        c.wait()


def early(level, vel, cross, inner, hi, lo, after):
    planes, rows, cols = level.shape
    ext = (planes + 2 * W, rows + SUB, cols)
    halo = (3 * (W - 1), rows, cols)
    return pl.pallas_call(
        early_kernel,
        out_shape=(
            near(*ext), near(*ext), near(*vel.shape), near(*halo), near(*halo), near(3, planes, SUB, cols)
        ),
        in_specs=[VMEM, FAR, LOOSE, LOOSE, VMEM, VMEM, LOOSE],
        out_specs=(VMEM,) * 6,
        scratch_shapes=[pltpu.SemaphoreType.DMA((2, 2)), pltpu.SemaphoreType.DMA((planes,))],
        compiler_params=params(20),
        name="early",
    )(*resident(level), *distant(vel), cross, inner, *resident(hi, lo), after)


def second_kernel(
    flag, f0, f1, vel, hcross, hinner, edge, ccross, cinner,
    out, level_out, f0_out, f1_out, sums, stage, sem, sent, *, scale,
):
    layers, all_rows, cols = f0.shape
    planes, rows = layers - 2 * W, all_rows - SUB
    nt = all_rows // SUB
    own_tiles = rows // SUB
    even = is_even()
    sides = ((hcross, ccross, even), (hinner, cinner, jnp.logical_not(even)))

    for _, corner, low in sides:
        zf = jnp.where(low, planes + W, planes)
        for j in range(W):
            f0_out[zf + j, rows : rows + SUB] = corner[j]

    def step(src, dst, t):
        reach = STEPS - t
        row_tiles = nt if reach else own_tiles

        def own(z, c):
            own_layer(src, dst, z, row_tiles, vel, edge)
            return c

        if t == 1:
            lax.fori_loop(0, 2, lambda n, c: own(n * (planes - 1), c), 0)
        else:
            lax.fori_loop(0, planes, own, 0)

        for halo, corner, low in sides:
            skip = jnp.where(low, W - 1 - reach, 0)
            base = jnp.where(low, -reach, planes)

            def outside(n, c):
                def speed(k, i, js):
                    at = (W - 1) * k + skip + n
                    if i == own_tiles:
                        return corner[W + at, :, js]
                    return halo[at, i * SUB : (i + 1) * SUB, js]

                layer(src, dst, base + n, row_tiles, speed)
                return c

            if reach:
                lax.fori_loop(0, reach, outside, 0)

    src, dst = f0_out, f1_out
    for t in range(1, STEPS + 1):
        step(src, dst, t)
        src, dst = dst, src

    store = pltpu.make_async_copy(src.at[pl.ds(0, planes), pl.ds(0, rows), :], level_out, sem)
    store.start()
    render(src, planes, rows, cols, flag[lax.axis_index("depth")], scale, sums)
    for c in spread(sums, out, stage, sent):
        c.wait()
    store.wait()


def second(flag, state, corners, scale, dests):
    ext = state[0].shape
    _, planes, rows, cols = state[2].shape
    packed = (dests, 3 * rows * cols // dests // LANES, LANES)
    return pl.pallas_call(
        functools.partial(second_kernel, scale=scale),
        out_shape=(
            pltpu.HBM(packed, jnp.float32),
            pltpu.HBM((planes, rows, cols), jnp.float32),
            near(*ext),
            near(*ext),
        ),
        in_specs=[SMEM] + [VMEM] * 8,
        out_specs=(FAR, FAR, VMEM, VMEM),
        input_output_aliases={1: 2, 2: 3},
        scratch_shapes=[
            pltpu.VMEM((3, rows, cols), jnp.float32),
            pltpu.VMEM(packed, jnp.float32),
            pltpu.SemaphoreType.DMA,
            pltpu.SemaphoreType.DMA((dests,)),
        ],
        compiler_params=params(20),
        name="second",
    )(flag, *resident(*state, *corners))[:2]


def composite_kernel(rank, parts, out):
    dests, stacked, _ = parts.shape
    part = stacked // 3
    _, rows, width = out.shape
    groups = rows // part
    for i in range(part // SUB):
        r = slice(i * SUB, (i + 1) * SUB)
        logs = [parts[e, 2 * part + i * SUB : 2 * part + (i + 1) * SUB, :] for e in range(dests)]
        q = g = total = None
        for b in range(dests):
            earlier = jnp.zeros((SUB, LANES), jnp.float32)
            for e in range(dests):
                if e != b:
                    earlier = earlier + jnp.where(rank[e] < rank[b], 1.0, 0.0) * logs[e]
            front = jnp.exp(earlier)
            qb = front * parts[b, r, :]
            gb = front * parts[b, part + i * SUB : part + (i + 1) * SUB, :]
            q = qb if q is None else q + qb
            g = gb if g is None else g + gb
            total = logs[b] if total is None else total + logs[b]
        alpha = 1.0 - jnp.exp(total)
        for ch, value in enumerate((0.5 * (alpha + q), g, 0.5 * (alpha - q), alpha)):
            for n in range(groups):
                piece = pltpu.roll(value, (LANES - n * width) % LANES, 1) if n else value
                out[ch, n * part + i * SUB : n * part + (i + 1) * SUB, :] = piece[:, :width]


def composite(rank, parts, rows, width):
    return pl.pallas_call(
        composite_kernel,
        out_shape=f32(4, rows, width),
        in_specs=[SMEM, VMEM],
        out_specs=VMEM,
        compiler_params=params(6),
        name="composite",
    )(rank, *resident(parts))


def program(level_set, velocity, view_flag, slab_rank):
    planes, rows, cols = level_set.shape
    depth = lax.axis_size("depth")
    image = lax.axis_size("image")
    scale = 2.0 / (planes * depth)
    width = cols // depth

    swap_inner = [(i, i ^ 1) for i in range(depth)]
    swap_cross = [p for i in range(1, depth - 1, 2) for p in ((i, i + 1), (i + 1, i))]
    up = [(i, i + 1) for i in range(image - 1)]
    down = [(b, a) for a, b in up]

    cross, inner = depth_pack(level_set, velocity)
    cross = lax.ppermute(cross, "depth", swap_cross)
    inner = lax.ppermute(inner, "depth", swap_inner)
    to_up, to_down = image_pack(level_set, velocity)
    lo = lax.ppermute(to_up, "image", up)
    hi = lax.ppermute(to_down, "image", down)
    ccross, cinner = corner_pack(hi, lo)
    state = early(level_set, velocity, cross, inner, hi, lo, ccross)
    ccross = lax.ppermute(ccross, "depth", swap_cross)
    cinner = lax.ppermute(cinner, "depth", swap_inner)

    packed = first(level_set, view_flag, to_up, scale, depth)
    parts = lax.all_to_all(packed, "depth", 0, 0, tiled=True)
    packed2, level_next = second(view_flag, state, (ccross, cinner), scale, depth)
    parts2 = lax.all_to_all(packed2, "depth", 0, 0, tiled=True)
    image_first = composite(slab_rank, parts, rows, width)
    image_second = composite(slab_rank, parts2, rows, width)
    return (image_first, image_second, level_next)


def solution(mesh):
    placed = (P("depth", "image", None), P(None, "depth", "image", None), P(), P())
    return jax.shard_map(
        program,
        mesh=mesh,
        in_specs=placed,
        out_specs=(P(None, "image", "depth"), P(None, "image", "depth"), P("depth", "image", None)),
        check_vma=False,
    )
```

```python
import functools

import jax
import jax.numpy as jnp
from jax import lax
from jax.experimental import pallas as pl
from jax.experimental.pallas import tpu as pltpu
from jax.sharding import PartitionSpec as P


STEPS = 4
step_size = 0.3
LANES = 128
SUB = 8
EARLY = 3
W = STEPS

VMEM = pl.BlockSpec(memory_space=pltpu.VMEM)
SMEM = pl.BlockSpec(memory_space=pltpu.SMEM)
FAR = pl.BlockSpec(memory_space=pltpu.HBM)
LOOSE = pl.BlockSpec(memory_space=pl.ANY)


def f32(*shape):
    return jax.ShapeDtypeStruct(shape, jnp.float32)


def near(*shape):
    return pltpu.VMEM(shape, jnp.float32)


def resident(*arrays):
    return [pltpu.with_memory_space_constraint(a, pltpu.VMEM) for a in arrays]


def params(mib=None):
    if mib is None:
        return pltpu.CompilerParams()
    return pltpu.CompilerParams(vmem_limit_bytes=mib * 2**20)


def distant(*arrays):
    return [pltpu.with_memory_space_constraint(a, pltpu.HBM) for a in arrays]


def is_even():
    return lax.rem(lax.axis_index("depth"), 2) == 0


def depth_pack_kernel(level, vel, cross, inner, sems):
    planes = level.shape[0]
    even = is_even()
    copies = []
    for n, (out, to_low) in enumerate(((cross, even), (inner, jnp.logical_not(even)))):
        z0 = jnp.where(to_low, 0, planes - W)
        v0 = jnp.where(to_low, 0, planes - W + 1)
        copies.append(pltpu.make_async_copy(level.at[pl.ds(z0, W)], out.at[pl.ds(0, W)], sems.at[n, 0]))
        for k in range(3):
            copies.append(
                pltpu.make_async_copy(
                    vel.at[k, pl.ds(v0, W - 1)],
                    out.at[pl.ds(W + (W - 1) * k, W - 1)],
                    sems.at[n, k + 1],
                )
            )
    for c in copies:
        c.start()
    for c in copies:
        c.wait()


def depth_pack(level, vel):
    _, rows, cols = level.shape
    shape = near(W + 3 * (W - 1), rows, cols)
    return pl.pallas_call(
        depth_pack_kernel,
        out_shape=(shape, shape),
        in_specs=[FAR, FAR],
        out_specs=(VMEM, VMEM),
        scratch_shapes=[pltpu.SemaphoreType.DMA((2, 4))],
        compiler_params=params(6),
        name="depth_pack",
    )(*distant(level, vel))


HALO_ROWS = W + 3 * (W - 1)


def row_span(z, k=None):
    start = z * HALO_ROWS + (0 if k is None else W + (W - 1) * k)
    return slice(start, start + (W if k is None else W - 1))


def image_pack_kernel(level, vel, up, down, lev, ve, sems):
    planes, rows, _ = level.shape
    copies = []
    for s, r0 in enumerate((0, rows - SUB)):
        copies.append(pltpu.make_async_copy(level.at[:, pl.ds(r0, SUB), :], lev.at[s], sems.at[s, 0]))
        copies.append(pltpu.make_async_copy(vel.at[:, :, pl.ds(r0, SUB), :], ve.at[s], sems.at[s, 1]))
    for c in copies:
        c.start()
    for c in copies:
        c.wait()

    for z in range(planes):
        down[row_span(z)] = lev[0, z, 0:W]
        up[row_span(z)] = lev[1, z, SUB - W : SUB]
        for k in range(3):
            down[row_span(z, k)] = ve[0, k, z, 0 : W - 1]
            up[row_span(z, k)] = ve[1, k, z, SUB - W + 1 : SUB]


def image_pack(level, vel):
    planes, _, cols = level.shape
    shape = near(planes * HALO_ROWS, cols)
    return pl.pallas_call(
        image_pack_kernel,
        out_shape=(shape, shape),
        in_specs=[FAR, FAR],
        out_specs=(VMEM, VMEM),
        scratch_shapes=[
            pltpu.VMEM((2, planes, SUB, cols), jnp.float32),
            pltpu.VMEM((2, 3, planes, SUB, cols), jnp.float32),
            pltpu.SemaphoreType.DMA((2, 2)),
        ],
        compiler_params=params(6),
        name="image_pack",
    )(*distant(level, vel))


def put_row_halos(field, speeds, hi, lo, z):
    field[0:W] = hi[row_span(z)]
    field[W:SUB] = lo[row_span(z)]
    for k, speed in enumerate(speeds):
        speed[...] = jnp.zeros(speed.shape, jnp.float32)
        speed[0 : W - 1] = hi[row_span(z, k)]
        speed[SUB - W + 1 : SUB] = lo[row_span(z, k)]


def corner_pack_kernel(hi, lo, cross, inner):
    planes = hi.shape[0] // HALO_ROWS
    even = is_even()

    def pack(low, high):
        for out, first, skip in ((low, 0, 0), (high, planes - W, 1)):
            for j in range(W):
                at = j - skip
                speeds = []
                if 0 <= at < W - 1:
                    speeds = [out.at[W + (W - 1) * k + at] for k in range(3)]
                put_row_halos(out.at[j], speeds, hi, lo, first + j)

    @pl.when(even)
    def _():
        pack(cross, inner)

    @pl.when(jnp.logical_not(even))
    def _():
        pack(inner, cross)


def corner_pack(hi, lo):
    shape = near(W + 3 * (W - 1), SUB, hi.shape[-1])
    return pl.pallas_call(
        corner_pack_kernel,
        out_shape=(shape, shape),
        in_specs=[VMEM, VMEM],
        out_specs=(VMEM, VMEM),
        compiler_params=params(6),
        name="corner_pack",
    )(*resident(hi, lo))


def render(field, planes, rows, cols, flag, scale, sums):
    reverse = flag != 0
    sign = jnp.where(reverse, 1.0, -1.0).astype(jnp.float32)

    def tile(i, c):
        r0 = pl.multiple_of(i * SUB, SUB)
        total = jnp.zeros((SUB, cols), jnp.float32)
        last = jnp.ones((SUB, cols), jnp.float32)
        q = jnp.zeros((SUB, cols), jnp.float32)
        g = jnp.zeros((SUB, cols), jnp.float32)
        step = sign * scale
        for z in range(planes):
            f = field[z, pl.ds(r0, SUB), :]
            e = jnp.exp(-f * f)
            total = total + e * step
            now = jnp.exp(total)
            weight = now - last
            last = now
            q = q + weight * jnp.tanh(f)
            g = g + weight * e
        logs = -sign * total
        factor = jnp.where(reverse, jnp.exp(logs), -1.0)
        sums[0, pl.ds(r0, SUB), :] = q * factor
        sums[1, pl.ds(r0, SUB), :] = g * factor
        sums[2, pl.ds(r0, SUB), :] = logs
        return c

    lax.fori_loop(0, rows // SUB, tile, 0)


def spread(sums, out, stage, sem):
    _, rows, cols = sums.shape
    dests = out.shape[0]
    copies = []
    width = cols // dests
    groups = LANES // width
    part = rows // groups
    lane = lax.broadcasted_iota(jnp.int32, (part, LANES), 1)
    for d in range(dests):
        j, offset = divmod(d * width, LANES)
        for ch in range(3):
            value = None
            for n in range(groups):
                piece = sums[ch, n * part : (n + 1) * part, j * LANES : (j + 1) * LANES]
                shift = (n * width - offset) % LANES
                if shift:
                    piece = pltpu.roll(piece, shift, 1)
                value = piece if value is None else jnp.where(lane < n * width, value, piece)
            stage[d, ch * part : (ch + 1) * part, :] = value
        copies.append(pltpu.make_async_copy(stage.at[d], out.at[d], sem.at[d]))
        copies[-1].start()
    return copies


def first_kernel(flag, level, after, out, sums, stage, sent, *, scale):
    planes, rows, cols = level.shape
    render(level, planes, rows, cols, flag[lax.axis_index("depth")], scale, sums)
    for c in spread(sums, out, stage, sent):
        c.wait()


def first(level, flag, after, scale, dests):
    _, rows, cols = level.shape
    packed = (dests, 3 * rows * cols // dests // LANES, LANES)
    return pl.pallas_call(
        functools.partial(first_kernel, scale=scale),
        out_shape=pltpu.HBM(packed, jnp.float32),
        in_specs=[SMEM, VMEM, LOOSE],
        out_specs=FAR,
        scratch_shapes=[
            pltpu.VMEM((3, rows, cols), jnp.float32),
            pltpu.VMEM(packed, jnp.float32),
            pltpu.SemaphoreType.DMA((dests,)),
        ],
        compiler_params=params(6),
        name="first",
    )(flag, *resident(level), after)


def side(tiles, j, lane, up):
    n = len(tiles)
    own = pltpu.roll(tiles[j], 1 if not up else LANES - 1, 1)
    k = j + 1 if up else j - 1
    if 0 <= k < n:
        other = pltpu.roll(tiles[k], 1 if not up else LANES - 1, 1)
    else:
        other = jnp.zeros_like(own)
    return jnp.where(lane == (LANES - 1 if up else 0), other, own)


def layer(src, dst, z, tiles_done, speed):
    layers, all_rows, cols = src.shape
    nt = all_rows // SUB
    nl = cols // LANES
    zi = jnp.where(z < 0, z + layers, z)
    zl = jnp.where(z < 1, z - 1 + layers, z - 1)
    zh = jnp.where(z < -1, z + 1 + layers, z + 1)
    sub = lax.broadcasted_iota(jnp.int32, (SUB, LANES), 0)
    lane = lax.broadcasted_iota(jnp.int32, (SUB, LANES), 1)
    first_sub = sub == 0
    last_sub = sub == SUB - 1
    for i in tiles_done:
        r = slice(i * SUB, (i + 1) * SUB)
        ru = slice((i + 1) % nt * SUB, ((i + 1) % nt + 1) * SUB)
        rd = slice((i - 1) % nt * SUB, ((i - 1) % nt + 1) * SUB)
        tiles = [src[zi, r, j * LANES : (j + 1) * LANES] for j in range(nl)]
        for j in range(nl):
            js = slice(j * LANES, (j + 1) * LANES)
            f = tiles[j]
            below = src[zi, rd, js]
            above = src[zi, ru, js]
            lows = (
                lambda: src[zl, r, js],
                lambda: jnp.where(first_sub, pltpu.roll(below, 1, 0), pltpu.roll(f, 1, 0)),
                lambda: side(tiles, j, lane, False),
            )
            highs = (
                lambda: src[zh, r, js],
                lambda: jnp.where(last_sub, pltpu.roll(above, SUB - 1, 0), pltpu.roll(f, SUB - 1, 0)),
                lambda: side(tiles, j, lane, True),
            )
            rate = None
            for k in range(3):
                u = speed(k, i, js)
                upwind = jnp.where(u > 0.0, lows[k](), highs[k]())
                term = jnp.abs(u) * (upwind - f)
                rate = term if rate is None else rate + term
            dst[zi, r, js] = f + step_size * rate


def own_layer(src, dst, z, row_tiles, vel, edge):
    own_tiles = vel.shape[2] // SUB

    def speed(k, i, js):
        if i == own_tiles:
            return edge[k, z, :, js]
        return vel[k, z, i * SUB : (i + 1) * SUB, js]

    layer(src, dst, z, row_tiles, speed)


def stage_kernel(level, speeds, f0, f1, vel, arrived):
    planes, rows, _ = level.shape
    streams = [
        pltpu.make_async_copy(speeds.at[:, z], vel.at[:, z], arrived.at[z]) for z in range(planes)
    ]
    for c in streams[1:-1] + [streams[0], streams[-1]]:
        c.start()

    def fill(z, c):
        f0[z, 0:rows] = level[z]
        return c

    lax.fori_loop(0, planes, fill, 0)

    def arriving(z, c):
        pltpu.make_async_copy(speeds.at[:, z], vel.at[:, z], arrived.at[z]).wait()
        own_layer(f0, f1, z, range(1, rows // SUB - 1), vel, None)
        return c

    lax.fori_loop(1, planes - 1, arriving, 0)
    streams[0].wait()
    streams[-1].wait()


def stage(level, vel):
    planes, rows, cols = level.shape
    ext = (planes + 2 * W, rows + SUB, cols)
    return pl.pallas_call(
        stage_kernel,
        out_shape=(near(*ext), near(*ext), near(*vel.shape)),
        in_specs=[VMEM, FAR],
        out_specs=(VMEM,) * 3,
        scratch_shapes=[pltpu.SemaphoreType.DMA((planes,))],
        compiler_params=params(16),
        name="stage",
    )(*resident(level), *distant(vel))


def early_kernel(
    f0_in, f1_in, vel, cross, inner, hi, lo, after, f0, f1, hcross, hinner, edge, sems
):
    layers, all_rows, _ = f0.shape
    planes, rows = layers - 2 * W, all_rows - SUB
    own_tiles = rows // SUB
    even = is_even()
    copies = []
    for n, (src, halo, low) in enumerate(((cross, hcross, even), (inner, hinner, jnp.logical_not(even)))):
        zf = jnp.where(low, planes + W, planes)
        copies.append(
            pltpu.make_async_copy(
                src.at[pl.ds(0, W)], f0.at[pl.ds(zf, W), pl.ds(0, rows), :], sems.at[n, 0]
            )
        )
        copies.append(pltpu.make_async_copy(src.at[pl.ds(W, 3 * (W - 1))], halo, sems.at[n, 1]))
    for c in copies:
        c.start()
    for z in range(planes):
        put_row_halos(f0.at[z, rows : rows + SUB], [edge.at[k, z] for k in range(3)], hi, lo, z)

    src, dst = f0, f1
    for t in range(1, EARLY + 1):
        done = (0, own_tiles - 1, own_tiles) if t == 1 else range(own_tiles + 1)

        def own(z, c):
            own_layer(src, dst, z, done, vel, edge)
            return c

        lax.fori_loop(t, planes - t, own, 0)
        src, dst = dst, src
    for c in copies:
        c.wait()


def early(staged, cross, inner, hi, lo, after):
    ext = staged[0].shape
    _, planes, rows, cols = staged[2].shape
    halo = (3 * (W - 1), rows, cols)
    out = pl.pallas_call(
        early_kernel,
        out_shape=(near(*ext), near(*ext), near(*halo), near(*halo), near(3, planes, SUB, cols)),
        in_specs=[VMEM, VMEM, VMEM, LOOSE, LOOSE, VMEM, VMEM, LOOSE],
        out_specs=(VMEM,) * 5,
        input_output_aliases={0: 0, 1: 1},
        scratch_shapes=[pltpu.SemaphoreType.DMA((2, 2))],
        compiler_params=params(20),
        name="early",
    )(*resident(*staged), cross, inner, *resident(hi, lo), after)
    return (out[0], out[1], staged[2], *out[2:])


def second_kernel(
    flag, f0, f1, vel, hcross, hinner, edge, ccross, cinner,
    out, level_out, f0_out, f1_out, sums, stage, sem, sent, *, scale,
):
    layers, all_rows, cols = f0.shape
    planes, rows = layers - 2 * W, all_rows - SUB
    nt = all_rows // SUB
    own_tiles = rows // SUB
    even = is_even()
    sides = ((hcross, ccross, even), (hinner, cinner, jnp.logical_not(even)))

    for _, corner, low in sides:
        zf = jnp.where(low, planes + W, planes)
        for j in range(W):
            f0_out[zf + j, rows : rows + SUB] = corner[j]

    def step(src, dst, t):
        reach = STEPS - t
        row_tiles = range(nt if reach else own_tiles)

        def own(z, c):
            own_layer(src, dst, z, row_tiles, vel, edge)
            return c

        if t <= EARLY:
            lax.fori_loop(0, 2 * t, lambda n, c: own(jnp.where(n < t, n, n + planes - 2 * t), c), 0)
        else:
            lax.fori_loop(0, planes, own, 0)

        for halo, corner, low in sides:
            skip = jnp.where(low, W - 1 - reach, 0)
            base = jnp.where(low, -reach, planes)

            def outside(n, c):
                def speed(k, i, js):
                    at = (W - 1) * k + skip + n
                    if i == own_tiles:
                        return corner[W + at, :, js]
                    return halo[at, i * SUB : (i + 1) * SUB, js]

                layer(src, dst, base + n, row_tiles, speed)
                return c

            if reach:
                lax.fori_loop(0, reach, outside, 0)

    src, dst = f0_out, f1_out
    for t in range(1, STEPS + 1):
        step(src, dst, t)
        src, dst = dst, src

    store = pltpu.make_async_copy(src.at[pl.ds(0, planes), pl.ds(0, rows), :], level_out, sem)
    store.start()
    render(src, planes, rows, cols, flag[lax.axis_index("depth")], scale, sums)
    for c in spread(sums, out, stage, sent):
        c.wait()
    store.wait()


def second(flag, state, corners, scale, dests):
    ext = state[0].shape
    _, planes, rows, cols = state[2].shape
    packed = (dests, 3 * rows * cols // dests // LANES, LANES)
    return pl.pallas_call(
        functools.partial(second_kernel, scale=scale),
        out_shape=(
            pltpu.HBM(packed, jnp.float32),
            pltpu.HBM((planes, rows, cols), jnp.float32),
            near(*ext),
            near(*ext),
        ),
        in_specs=[SMEM] + [VMEM] * 8,
        out_specs=(FAR, FAR, VMEM, VMEM),
        input_output_aliases={1: 2, 2: 3},
        scratch_shapes=[
            pltpu.VMEM((3, rows, cols), jnp.float32),
            pltpu.VMEM(packed, jnp.float32),
            pltpu.SemaphoreType.DMA,
            pltpu.SemaphoreType.DMA((dests,)),
        ],
        compiler_params=params(20),
        name="second",
    )(flag, *resident(*state, *corners))[:2]


def composite_kernel(rank, parts, out):
    dests, stacked, _ = parts.shape
    part = stacked // 3
    _, rows, width = out.shape
    groups = rows // part
    for i in range(part // SUB):
        r = slice(i * SUB, (i + 1) * SUB)
        logs = [parts[e, 2 * part + i * SUB : 2 * part + (i + 1) * SUB, :] for e in range(dests)]
        q = g = total = None
        for b in range(dests):
            earlier = jnp.zeros((SUB, LANES), jnp.float32)
            for e in range(dests):
                if e != b:
                    earlier = earlier + jnp.where(rank[e] < rank[b], 1.0, 0.0) * logs[e]
            front = jnp.exp(earlier)
            qb = front * parts[b, r, :]
            gb = front * parts[b, part + i * SUB : part + (i + 1) * SUB, :]
            q = qb if q is None else q + qb
            g = gb if g is None else g + gb
            total = logs[b] if total is None else total + logs[b]
        alpha = 1.0 - jnp.exp(total)
        for ch, value in enumerate((0.5 * (alpha + q), g, 0.5 * (alpha - q), alpha)):
            for n in range(groups):
                piece = pltpu.roll(value, (LANES - n * width) % LANES, 1) if n else value
                out[ch, n * part + i * SUB : n * part + (i + 1) * SUB, :] = piece[:, :width]


def composite(rank, parts, rows, width):
    return pl.pallas_call(
        composite_kernel,
        out_shape=f32(4, rows, width),
        in_specs=[SMEM, VMEM],
        out_specs=VMEM,
        compiler_params=params(6),
        name="composite",
    )(rank, *resident(parts))


def program(level_set, velocity, view_flag, slab_rank):
    planes, rows, cols = level_set.shape
    depth = lax.axis_size("depth")
    image = lax.axis_size("image")
    scale = 2.0 / (planes * depth)
    width = cols // depth

    swap_inner = [(i, i ^ 1) for i in range(depth)]
    swap_cross = [p for i in range(1, depth - 1, 2) for p in ((i, i + 1), (i + 1, i))]
    up = [(i, i + 1) for i in range(image - 1)]
    down = [(b, a) for a, b in up]

    cross, inner = depth_pack(level_set, velocity)
    cross = lax.ppermute(cross, "depth", swap_cross)
    inner = lax.ppermute(inner, "depth", swap_inner)
    to_up, to_down = image_pack(level_set, velocity)
    lo = lax.ppermute(to_up, "image", up)
    hi = lax.ppermute(to_down, "image", down)
    ccross, cinner = corner_pack(hi, lo)
    staged = stage(level_set, velocity)
    state = early(staged, cross, inner, hi, lo, ccross)
    ccross = lax.ppermute(ccross, "depth", swap_cross)
    cinner = lax.ppermute(cinner, "depth", swap_inner)

    packed = first(level_set, view_flag, to_up, scale, depth)
    parts = lax.all_to_all(packed, "depth", 0, 0, tiled=True)
    packed2, level_next = second(view_flag, state, (ccross, cinner), scale, depth)
    parts2 = lax.all_to_all(packed2, "depth", 0, 0, tiled=True)
    image_first = composite(slab_rank, parts, rows, width)
    image_second = composite(slab_rank, parts2, rows, width)
    return (image_first, image_second, level_next)


def solution(mesh):
    placed = (P("depth", "image", None), P(None, "depth", "image", None), P(), P())
    return jax.shard_map(
        program,
        mesh=mesh,
        in_specs=placed,
        out_specs=(P(None, "image", "depth"), P(None, "image", "depth"), P("depth", "image", None)),
        check_vma=False,
    )
```

```python
import functools

import jax
import jax.numpy as jnp
from jax import lax
from jax.experimental import pallas as pl
from jax.experimental.pallas import tpu as pltpu
from jax.sharding import PartitionSpec as P


STEPS = 4
step_size = 0.3
LANES = 128
SUB = 8
EARLY = STEPS
STAGED = 3
W = STEPS

VMEM = pl.BlockSpec(memory_space=pltpu.VMEM)
SMEM = pl.BlockSpec(memory_space=pltpu.SMEM)
FAR = pl.BlockSpec(memory_space=pltpu.HBM)
LOOSE = pl.BlockSpec(memory_space=pl.ANY)


def f32(*shape):
    return jax.ShapeDtypeStruct(shape, jnp.float32)


def near(*shape):
    return pltpu.VMEM(shape, jnp.float32)


def resident(*arrays):
    return [pltpu.with_memory_space_constraint(a, pltpu.VMEM) for a in arrays]


def params(mib=None):
    if mib is None:
        return pltpu.CompilerParams()
    return pltpu.CompilerParams(vmem_limit_bytes=mib * 2**20)


def distant(*arrays):
    return [pltpu.with_memory_space_constraint(a, pltpu.HBM) for a in arrays]


def is_even():
    return lax.rem(lax.axis_index("depth"), 2) == 0


def depth_pack_kernel(level, vel, cross, inner, sems):
    planes = level.shape[0]
    even = is_even()
    copies = []
    for n, (out, to_low) in enumerate(((cross, even), (inner, jnp.logical_not(even)))):
        z0 = jnp.where(to_low, 0, planes - W)
        v0 = jnp.where(to_low, 0, planes - W + 1)
        copies.append(pltpu.make_async_copy(level.at[pl.ds(z0, W)], out.at[pl.ds(0, W)], sems.at[n, 0]))
        for k in range(3):
            copies.append(
                pltpu.make_async_copy(
                    vel.at[k, pl.ds(v0, W - 1)],
                    out.at[pl.ds(W + (W - 1) * k, W - 1)],
                    sems.at[n, k + 1],
                )
            )
    for c in copies:
        c.start()
    for c in copies:
        c.wait()


def depth_pack(level, vel):
    _, rows, cols = level.shape
    shape = near(W + 3 * (W - 1), rows, cols)
    return pl.pallas_call(
        depth_pack_kernel,
        out_shape=(shape, shape),
        in_specs=[FAR, FAR],
        out_specs=(VMEM, VMEM),
        scratch_shapes=[pltpu.SemaphoreType.DMA((2, 4))],
        compiler_params=params(6),
        name="depth_pack",
    )(*distant(level, vel))


HALO_ROWS = W + 3 * (W - 1)


def row_span(z, k=None):
    start = z * HALO_ROWS + (0 if k is None else W + (W - 1) * k)
    return slice(start, start + (W if k is None else W - 1))


def image_pack_kernel(level, vel, up, down, lev, ve, sems):
    planes, rows, _ = level.shape
    copies = []
    for s, r0 in enumerate((0, rows - SUB)):
        copies.append(pltpu.make_async_copy(level.at[:, pl.ds(r0, SUB), :], lev.at[s], sems.at[s, 0]))
        copies.append(pltpu.make_async_copy(vel.at[:, :, pl.ds(r0, SUB), :], ve.at[s], sems.at[s, 1]))
    for c in copies:
        c.start()
    for c in copies:
        c.wait()

    for z in range(planes):
        down[row_span(z)] = lev[0, z, 0:W]
        up[row_span(z)] = lev[1, z, SUB - W : SUB]
        for k in range(3):
            down[row_span(z, k)] = ve[0, k, z, 0 : W - 1]
            up[row_span(z, k)] = ve[1, k, z, SUB - W + 1 : SUB]


def image_pack(level, vel):
    planes, _, cols = level.shape
    shape = near(planes * HALO_ROWS, cols)
    return pl.pallas_call(
        image_pack_kernel,
        out_shape=(shape, shape),
        in_specs=[FAR, FAR],
        out_specs=(VMEM, VMEM),
        scratch_shapes=[
            pltpu.VMEM((2, planes, SUB, cols), jnp.float32),
            pltpu.VMEM((2, 3, planes, SUB, cols), jnp.float32),
            pltpu.SemaphoreType.DMA((2, 2)),
        ],
        compiler_params=params(6),
        name="image_pack",
    )(*distant(level, vel))


def put_row_halos(field, speeds, hi, lo, z):
    field[0:W] = hi[row_span(z)]
    field[W:SUB] = lo[row_span(z)]
    for k, speed in enumerate(speeds):
        speed[...] = jnp.zeros(speed.shape, jnp.float32)
        speed[0 : W - 1] = hi[row_span(z, k)]
        speed[SUB - W + 1 : SUB] = lo[row_span(z, k)]


def corner_pack_kernel(hi, lo, cross, inner):
    planes = hi.shape[0] // HALO_ROWS
    even = is_even()

    def pack(low, high):
        for out, first, skip in ((low, 0, 0), (high, planes - W, 1)):
            for j in range(W):
                at = j - skip
                speeds = []
                if 0 <= at < W - 1:
                    speeds = [out.at[W + (W - 1) * k + at] for k in range(3)]
                put_row_halos(out.at[j], speeds, hi, lo, first + j)

    @pl.when(even)
    def _():
        pack(cross, inner)

    @pl.when(jnp.logical_not(even))
    def _():
        pack(inner, cross)


def corner_pack(hi, lo):
    shape = near(W + 3 * (W - 1), SUB, hi.shape[-1])
    return pl.pallas_call(
        corner_pack_kernel,
        out_shape=(shape, shape),
        in_specs=[VMEM, VMEM],
        out_specs=(VMEM, VMEM),
        compiler_params=params(6),
        name="corner_pack",
    )(*resident(hi, lo))


def render(field, planes, rows, cols, flag, scale, sums):
    reverse = flag != 0
    sign = jnp.where(reverse, 1.0, -1.0).astype(jnp.float32)

    def tile(i, c):
        r0 = pl.multiple_of(i * SUB, SUB)
        total = jnp.zeros((SUB, cols), jnp.float32)
        last = jnp.ones((SUB, cols), jnp.float32)
        q = jnp.zeros((SUB, cols), jnp.float32)
        g = jnp.zeros((SUB, cols), jnp.float32)
        step = sign * scale
        for z in range(planes):
            f = field[z, pl.ds(r0, SUB), :]
            e = jnp.exp(-f * f)
            total = total + e * step
            now = jnp.exp(total)
            weight = now - last
            last = now
            q = q + weight * jnp.tanh(f)
            g = g + weight * e
        logs = -sign * total
        factor = jnp.where(reverse, jnp.exp(logs), -1.0)
        sums[0, pl.ds(r0, SUB), :] = q * factor
        sums[1, pl.ds(r0, SUB), :] = g * factor
        sums[2, pl.ds(r0, SUB), :] = logs
        return c

    lax.fori_loop(0, rows // SUB, tile, 0)


def spread(sums, out, stage, sem):
    _, rows, cols = sums.shape
    dests = out.shape[0]
    copies = []
    width = cols // dests
    groups = LANES // width
    part = rows // groups
    lane = lax.broadcasted_iota(jnp.int32, (part, LANES), 1)
    for d in range(dests):
        j, offset = divmod(d * width, LANES)
        for ch in range(3):
            value = None
            for n in range(groups):
                piece = sums[ch, n * part : (n + 1) * part, j * LANES : (j + 1) * LANES]
                shift = (n * width - offset) % LANES
                if shift:
                    piece = pltpu.roll(piece, shift, 1)
                value = piece if value is None else jnp.where(lane < n * width, value, piece)
            stage[d, ch * part : (ch + 1) * part, :] = value
        copies.append(pltpu.make_async_copy(stage.at[d], out.at[d], sem.at[d]))
        copies[-1].start()
    return copies


def first_kernel(flag, level, after, out, sums, stage, sent, *, scale):
    planes, rows, cols = level.shape
    render(level, planes, rows, cols, flag[lax.axis_index("depth")], scale, sums)
    for c in spread(sums, out, stage, sent):
        c.wait()


def first(level, flag, after, scale, dests):
    _, rows, cols = level.shape
    packed = (dests, 3 * rows * cols // dests // LANES, LANES)
    return pl.pallas_call(
        functools.partial(first_kernel, scale=scale),
        out_shape=pltpu.HBM(packed, jnp.float32),
        in_specs=[SMEM, VMEM, LOOSE],
        out_specs=FAR,
        scratch_shapes=[
            pltpu.VMEM((3, rows, cols), jnp.float32),
            pltpu.VMEM(packed, jnp.float32),
            pltpu.SemaphoreType.DMA((dests,)),
        ],
        compiler_params=params(6),
        name="first",
    )(flag, *resident(level), after)


def side(tiles, j, lane, up):
    n = len(tiles)
    own = pltpu.roll(tiles[j], 1 if not up else LANES - 1, 1)
    k = j + 1 if up else j - 1
    if 0 <= k < n:
        other = pltpu.roll(tiles[k], 1 if not up else LANES - 1, 1)
    else:
        other = jnp.zeros_like(own)
    return jnp.where(lane == (LANES - 1 if up else 0), other, own)


def layer(src, dst, z, tiles_done, speed):
    layers, all_rows, cols = src.shape
    nt = all_rows // SUB
    nl = cols // LANES
    zi = jnp.where(z < 0, z + layers, z)
    zl = jnp.where(z < 1, z - 1 + layers, z - 1)
    zh = jnp.where(z < -1, z + 1 + layers, z + 1)
    sub = lax.broadcasted_iota(jnp.int32, (SUB, LANES), 0)
    lane = lax.broadcasted_iota(jnp.int32, (SUB, LANES), 1)
    first_sub = sub == 0
    last_sub = sub == SUB - 1
    for i in tiles_done:
        r = slice(i * SUB, (i + 1) * SUB)
        ru = slice((i + 1) % nt * SUB, ((i + 1) % nt + 1) * SUB)
        rd = slice((i - 1) % nt * SUB, ((i - 1) % nt + 1) * SUB)
        tiles = [src[zi, r, j * LANES : (j + 1) * LANES] for j in range(nl)]
        for j in range(nl):
            js = slice(j * LANES, (j + 1) * LANES)
            f = tiles[j]
            below = src[zi, rd, js]
            above = src[zi, ru, js]
            lows = (
                lambda: src[zl, r, js],
                lambda: jnp.where(first_sub, pltpu.roll(below, 1, 0), pltpu.roll(f, 1, 0)),
                lambda: side(tiles, j, lane, False),
            )
            highs = (
                lambda: src[zh, r, js],
                lambda: jnp.where(last_sub, pltpu.roll(above, SUB - 1, 0), pltpu.roll(f, SUB - 1, 0)),
                lambda: side(tiles, j, lane, True),
            )
            rate = None
            for k in range(3):
                u = speed(k, i, js)
                upwind = jnp.where(u > 0.0, lows[k](), highs[k]())
                term = jnp.abs(u) * (upwind - f)
                rate = term if rate is None else rate + term
            dst[zi, r, js] = f + step_size * rate


def own_layer(src, dst, z, row_tiles, vel, edge):
    own_tiles = vel.shape[2] // SUB

    def speed(k, i, js):
        if i == own_tiles:
            return edge[k, z, :, js]
        return vel[k, z, i * SUB : (i + 1) * SUB, js]

    layer(src, dst, z, row_tiles, speed)


def staged_tiles(t, own_tiles):
    return range(t, own_tiles - t) if t <= STAGED else range(0)


def stage_kernel(level, speeds, f0, f1, vel, filled, arrived):
    planes, rows, _ = level.shape
    own_tiles = rows // SUB
    fill = pltpu.make_async_copy(level, f0.at[pl.ds(0, planes), pl.ds(0, rows), :], filled)
    streams = [
        pltpu.make_async_copy(speeds.at[:, z], vel.at[:, z], arrived.at[z]) for z in range(planes)
    ]
    for c in [fill] + streams[1:-1] + [streams[0], streams[-1]]:
        c.start()
    fill.wait()

    src, dst = f0, f1
    for t in range(1, STAGED + 1):

        def own(z, c):
            if t == 1:
                pltpu.make_async_copy(speeds.at[:, z], vel.at[:, z], arrived.at[z]).wait()
            own_layer(src, dst, z, staged_tiles(t, own_tiles), vel, None)
            return c

        lax.fori_loop(t, planes - t, own, 0)
        src, dst = dst, src
    streams[0].wait()
    streams[-1].wait()


def stage(level, vel):
    planes, rows, cols = level.shape
    ext = (planes + 2 * W, rows + SUB, cols)
    return pl.pallas_call(
        stage_kernel,
        out_shape=(near(*ext), near(*ext), near(*vel.shape)),
        in_specs=[FAR, FAR],
        out_specs=(VMEM,) * 3,
        scratch_shapes=[pltpu.SemaphoreType.DMA, pltpu.SemaphoreType.DMA((planes,))],
        compiler_params=params(16),
        name="stage",
    )(*distant(level, vel))


def early_kernel(
    f0_in, f1_in, vel, cross, inner, hi, lo, after, f0, f1, hcross, hinner, edge, sems
):
    layers, all_rows, _ = f0.shape
    planes, rows = layers - 2 * W, all_rows - SUB
    own_tiles = rows // SUB
    even = is_even()
    copies = []
    for n, (src, halo, low) in enumerate(((cross, hcross, even), (inner, hinner, jnp.logical_not(even)))):
        zf = jnp.where(low, planes + W, planes)
        copies.append(
            pltpu.make_async_copy(
                src.at[pl.ds(0, W)], f0.at[pl.ds(zf, W), pl.ds(0, rows), :], sems.at[n, 0]
            )
        )
        copies.append(pltpu.make_async_copy(src.at[pl.ds(W, 3 * (W - 1))], halo, sems.at[n, 1]))
    for c in copies:
        c.start()
    for z in range(planes):
        put_row_halos(f0.at[z, rows : rows + SUB], [edge.at[k, z] for k in range(3)], hi, lo, z)

    src, dst = f0, f1
    for t in range(1, EARLY + 1):
        ready = staged_tiles(t, own_tiles)
        done = [i for i in range(own_tiles + (t < STEPS)) if i not in ready]

        def own(z, c):
            own_layer(src, dst, z, done, vel, edge)
            return c

        lax.fori_loop(t, planes - t, own, 0)
        src, dst = dst, src
    for c in copies:
        c.wait()


def early(staged, cross, inner, hi, lo, after):
    ext = staged[0].shape
    _, planes, rows, cols = staged[2].shape
    halo = (3 * (W - 1), rows, cols)
    out = pl.pallas_call(
        early_kernel,
        out_shape=(near(*ext), near(*ext), near(*halo), near(*halo), near(3, planes, SUB, cols)),
        in_specs=[VMEM, VMEM, VMEM, LOOSE, LOOSE, VMEM, VMEM, LOOSE],
        out_specs=(VMEM,) * 5,
        input_output_aliases={0: 0, 1: 1},
        scratch_shapes=[pltpu.SemaphoreType.DMA((2, 2))],
        compiler_params=params(20),
        name="early",
    )(*resident(*staged), cross, inner, *resident(hi, lo), after)
    return (out[0], out[1], staged[2], *out[2:])


def second_kernel(
    flag, f0, f1, vel, hcross, hinner, edge, ccross, cinner,
    out, level_out, f0_out, f1_out, sums, stage, sem, sent, *, scale,
):
    layers, all_rows, cols = f0.shape
    planes, rows = layers - 2 * W, all_rows - SUB
    nt = all_rows // SUB
    own_tiles = rows // SUB
    even = is_even()
    sides = ((hcross, ccross, even), (hinner, cinner, jnp.logical_not(even)))

    for _, corner, low in sides:
        zf = jnp.where(low, planes + W, planes)
        for j in range(W):
            f0_out[zf + j, rows : rows + SUB] = corner[j]

    def step(src, dst, t):
        reach = STEPS - t
        row_tiles = range(nt if reach else own_tiles)

        def own(z, c):
            own_layer(src, dst, z, row_tiles, vel, edge)
            return c

        if t <= EARLY:
            lax.fori_loop(0, 2 * t, lambda n, c: own(jnp.where(n < t, n, n + planes - 2 * t), c), 0)
        else:
            lax.fori_loop(0, planes, own, 0)

        for halo, corner, low in sides:
            skip = jnp.where(low, W - 1 - reach, 0)
            base = jnp.where(low, -reach, planes)

            def outside(n, c):
                def speed(k, i, js):
                    at = (W - 1) * k + skip + n
                    if i == own_tiles:
                        return corner[W + at, :, js]
                    return halo[at, i * SUB : (i + 1) * SUB, js]

                layer(src, dst, base + n, row_tiles, speed)
                return c

            if reach:
                lax.fori_loop(0, reach, outside, 0)

    src, dst = f0_out, f1_out
    for t in range(1, STEPS + 1):
        step(src, dst, t)
        src, dst = dst, src

    store = pltpu.make_async_copy(src.at[pl.ds(0, planes), pl.ds(0, rows), :], level_out, sem)
    store.start()
    render(src, planes, rows, cols, flag[lax.axis_index("depth")], scale, sums)
    for c in spread(sums, out, stage, sent):
        c.wait()
    store.wait()


def second(flag, state, corners, scale, dests):
    ext = state[0].shape
    _, planes, rows, cols = state[2].shape
    packed = (dests, 3 * rows * cols // dests // LANES, LANES)
    return pl.pallas_call(
        functools.partial(second_kernel, scale=scale),
        out_shape=(
            pltpu.HBM(packed, jnp.float32),
            pltpu.HBM((planes, rows, cols), jnp.float32),
            near(*ext),
            near(*ext),
        ),
        in_specs=[SMEM] + [VMEM] * 8,
        out_specs=(FAR, FAR, VMEM, VMEM),
        input_output_aliases={1: 2, 2: 3},
        scratch_shapes=[
            pltpu.VMEM((3, rows, cols), jnp.float32),
            pltpu.VMEM(packed, jnp.float32),
            pltpu.SemaphoreType.DMA,
            pltpu.SemaphoreType.DMA((dests,)),
        ],
        compiler_params=params(20),
        name="second",
    )(flag, *resident(*state, *corners))[:2]


def composite_kernel(rank, parts, out):
    dests, stacked, _ = parts.shape
    part = stacked // 3
    _, rows, width = out.shape
    groups = rows // part
    for i in range(part // SUB):
        r = slice(i * SUB, (i + 1) * SUB)
        logs = [parts[e, 2 * part + i * SUB : 2 * part + (i + 1) * SUB, :] for e in range(dests)]
        q = g = total = None
        for b in range(dests):
            earlier = jnp.zeros((SUB, LANES), jnp.float32)
            for e in range(dests):
                if e != b:
                    earlier = earlier + jnp.where(rank[e] < rank[b], 1.0, 0.0) * logs[e]
            front = jnp.exp(earlier)
            qb = front * parts[b, r, :]
            gb = front * parts[b, part + i * SUB : part + (i + 1) * SUB, :]
            q = qb if q is None else q + qb
            g = gb if g is None else g + gb
            total = logs[b] if total is None else total + logs[b]
        alpha = 1.0 - jnp.exp(total)
        for ch, value in enumerate((0.5 * (alpha + q), g, 0.5 * (alpha - q), alpha)):
            for n in range(groups):
                piece = pltpu.roll(value, (LANES - n * width) % LANES, 1) if n else value
                out[ch, n * part + i * SUB : n * part + (i + 1) * SUB, :] = piece[:, :width]


def composite(rank, parts, rows, width):
    return pl.pallas_call(
        composite_kernel,
        out_shape=f32(4, rows, width),
        in_specs=[SMEM, VMEM],
        out_specs=VMEM,
        compiler_params=params(6),
        name="composite",
    )(rank, *resident(parts))


def program(level_set, velocity, view_flag, slab_rank):
    planes, rows, cols = level_set.shape
    depth = lax.axis_size("depth")
    image = lax.axis_size("image")
    scale = 2.0 / (planes * depth)
    width = cols // depth

    swap_inner = [(i, i ^ 1) for i in range(depth)]
    swap_cross = [p for i in range(1, depth - 1, 2) for p in ((i, i + 1), (i + 1, i))]
    up = [(i, i + 1) for i in range(image - 1)]
    down = [(b, a) for a, b in up]

    cross, inner = depth_pack(level_set, velocity)
    cross = lax.ppermute(cross, "depth", swap_cross)
    inner = lax.ppermute(inner, "depth", swap_inner)
    to_up, to_down = image_pack(level_set, velocity)
    lo = lax.ppermute(to_up, "image", up)
    hi = lax.ppermute(to_down, "image", down)
    ccross, cinner = corner_pack(hi, lo)
    staged = stage(level_set, velocity)
    state = early(staged, cross, inner, hi, lo, ccross)
    ccross = lax.ppermute(ccross, "depth", swap_cross)
    cinner = lax.ppermute(cinner, "depth", swap_inner)

    packed = first(level_set, view_flag, to_up, scale, depth)
    parts = lax.all_to_all(packed, "depth", 0, 0, tiled=True)
    packed2, level_next = second(view_flag, state, (ccross, cinner), scale, depth)
    parts2 = lax.all_to_all(packed2, "depth", 0, 0, tiled=True)
    image_first = composite(slab_rank, parts, rows, width)
    image_second = composite(slab_rank, parts2, rows, width)
    return (image_first, image_second, level_next)


def solution(mesh):
    placed = (P("depth", "image", None), P(None, "depth", "image", None), P(), P())
    return jax.shard_map(
        program,
        mesh=mesh,
        in_specs=placed,
        out_specs=(P(None, "image", "depth"), P(None, "image", "depth"), P("depth", "image", None)),
        check_vma=False,
    )
```
